32 devices in a mesh: prow: 4 (over y, x), pcol: 8 (over z, core).
Axes of the slice: x: 2, y: 2, z: 4, core: 2. Of those that a mesh axis runs over, the one named last changes fastest.
Arguments:
- panel_t: float32 [8, 256, 4096], P('pcol', None, 'prow'), may hold values from -0.09375 to 0.09375
- ancestor: float32 [4096, 4096], P('prow', 'pcol'), as said below
- structure: int32 [8, 16], replicated, may hold values 0 or 1
- diag_inv: float32 [8, 256, 256], P('pcol'), may hold values from -6 to 6
Outputs:
- inverse_panel: float32 [2048, 4096], P('pcol', 'prow')
- inverse_diag: float32 [8, 256, 256], P('pcol')
The draws below stay inside these ranges and needn't reach their ends.
Inputs may be any that keep to these rules, and one draw needn't show every extreme that they name: ancestor is symmetric up to rounding.
All inputs are finite; a program needn't handle non-finite values.
Results may differ from the reference program's by a relative error of at most 0.00007.
Values sent between devices are 32-bit elements; how exact they have to be, the bound alone decides.
A program may use at most 128 MiB of HBM per device.

```python
import jax
import jax.numpy as jnp
from jax import lax

B = 256
S = 8
NA = 16
R = 4096


def draw_ancestor(key, part):
    first = jax.random.normal(jax.random.fold_in(key, 11), (R, R), jnp.float32)
    matrix = (first + first.T) * 0.7071
    return matrix


def place_ends(array, key, smallest, high):
    longest = array.shape.index(max(array.shape))
    spots = []
    for shift in (0, 1):
        where = [jax.random.randint(jax.random.fold_in(key, axis), (), 0, length) for axis, length in enumerate(array.shape)]
        where[longest] = (where[longest] + shift) % array.shape[longest]
        spots.append(tuple(where))
    return array.at[spots[0]].set(smallest).at[spots[1]].set(high)


def level_of(own_key, dims, split, smallest, top_value):
    def one(axis_at, parts):
        steps = jax.random.uniform(jax.random.fold_in(jax.random.fold_in(own_key, 6), axis_at), (parts,), jnp.float32, smallest / len(split), top_value / len(split))
        return jnp.repeat(jnp.exp(steps), dims[axis_at] // parts).reshape((-1,) + (1,) * (len(dims) - axis_at - 1))

    factor_of = one(*split[0])
    for cut in split[1:]:
        factor_of = factor_of * one(*cut)
    return factor_of


def gaussian(own_key, extent, spread, reach, split=(), held_as=jnp.bfloat16):
    values = jax.random.normal(own_key, extent, jnp.float32) * spread
    if len(split) > 0:
        values = level_of(own_key, extent, split, -0.22, 0.18) * values
    return jnp.clip(values, min=-reach, max=reach).astype(held_as)


def setup_inputs(seed: int = 0) -> dict:
    key_of = jax.random.split(jax.random.key(seed), 5)
    panel_t = gaussian(key_of[0], (S, B, R), R ** -0.5, 0.09375, ((0, 8), (2, 4)), jnp.float32)
    ancestor = draw_ancestor(jax.random.fold_in(key_of[4], 71), 0)
    structure = place_ends((jax.random.randint(key_of[2], (S, NA), 0, 4) < 3).astype(jnp.int32), jax.random.fold_in(key_of[2], 1), 0, 1)
    diag_inv = gaussian(key_of[3], (S, B, B), 1.0, 6.0, ((0, 8),), jnp.float32)
    return dict(panel_t=panel_t, ancestor=ancestor, structure=structure, diag_inv=diag_inv)


def reference(panel_t, ancestor, structure, diag_inv):
    mask = jnp.repeat(structure.astype(jnp.float32), B, axis=1)
    masked = panel_t * mask[:, None, :]
    flat = masked.reshape(S * B, R)
    inverse_panel = -jnp.dot(flat, ancestor, precision=lax.Precision.HIGHEST, preferred_element_type=jnp.float32)
    blocks = inverse_panel.reshape(S, B, R)
    inverse_diag = diag_inv - jnp.einsum("kbj,kcj->kbc", blocks, masked, precision=lax.Precision.HIGHEST)
    return inverse_panel, inverse_diag
```

```python
import functools

import jax
import jax.numpy as jnp
from jax import lax
from jax.experimental import pallas as pl
from jax.experimental.pallas import tpu as pltpu
from jax.sharding import PartitionSpec as P

MESH = pl.DeviceIdType.MESH
f32 = jnp.float32
bf16 = jnp.bfloat16


def split(x):
    hi = x.astype(bf16)
    return hi, (x - hi.astype(f32)).astype(bf16)


def product(x, w_hi, w_lo, dims):
    hi, lo = split(x)
    rows = x.shape[0]
    both = lax.dot_general(
        jnp.concatenate([hi, lo], axis=0), w_hi, dims, preferred_element_type=f32
    )
    return both[:rows] + (
        both[rows:] + lax.dot_general(hi, w_lo, dims, preferred_element_type=f32)
    )


def kernel(
    n, nz, g,
    st_ref, panel_ref, anc_ref, diag_ref, inv_ref, out_diag_ref,
    gath, part, rs, sums, fin, a_recv, a_hi, a_lo, m_hi, m_lo, dpart, drecv, dsum, dout,
    a_send_sem, a_recv_sem, right_sem, left_sem, gath_sem, part_sem, rs_sem,
    sum_sem, fin_sem, dp_sem, dr_sem, db_sem, do_sem,
):
    r = lax.axis_index("prow")
    me = lax.axis_index("pcol")
    z, c = me // g, me % g
    width = panel_ref.shape[1]
    ch = width // n
    nb = panel_ref.shape[2] // width
    cols = anc_ref.shape[1]

    def dev(row, plane):
        return (row, plane * g + c)

    def copy(src, dst, s, d, to):
        return pltpu.make_async_remote_copy(
            src_ref=src, dst_ref=dst, send_sem=s, recv_sem=d, device_id=to, device_id_type=MESH
        )

    barrier = pltpu.get_barrier_semaphore()
    for step in range(1, n * nz):
        other = lax.rem(r * nz + z + step, n * nz)
        pl.semaphore_signal(barrier, inc=1, device_id=dev(other // nz, other % nz), device_id_type=MESH)
    for o in range(1, g):
        pl.semaphore_signal(
            barrier, inc=1, device_id=(r, z * g + lax.rem(c + o, g)), device_id_type=MESH
        )

    mask = [st_ref[me, r * nb + j].astype(f32) for j in range(nb)]
    for q in range(n):
        for j in range(nb):
            at = slice(j * width, (j + 1) * width)
            gath[z, q, :, at] = panel_ref[0, q * ch : (q + 1) * ch, at] * mask[j]

    pl.semaphore_wait(barrier, n * nz - 1 + g - 1)

    def a_copy(o):
        return copy(
            anc_ref, a_recv.at[o - 1], a_send_sem.at[o - 1], a_recv_sem.at[o - 1],
            (r, z * g + lax.rem(c + o, g)),
        )

    for o in range(1, g):
        a_copy(o).start()

    def to_right(b, q):
        return copy(gath.at[b, q], gath.at[b, q], right_sem.at[b, q], gath_sem.at[b, q], dev(r, z + 1))

    def to_left(b, q):
        return copy(gath.at[b, q], gath.at[b, q], left_sem.at[b, q], gath_sem.at[b, q], dev(r, z - 1))

    def part_copy(b, q):
        return copy(part.at[b, q], rs.at[b, r], part_sem.at[b, q], rs_sem.at[b, r], dev(q, z))

    def sum_copy(b):
        return copy(sums.at[b], fin.at[r], sum_sem.at[b], fin_sem.at[r], dev(z, b))

    for q in range(n):
        @pl.when(z < nz - 1)
        def _():
            to_right(z, q).start()

        @pl.when(z > 0)
        def _():
            to_left(z, q).start()

    hi, lo = split(anc_ref[...])
    a_hi[c] = hi
    a_lo[c] = lo
    for q in range(n):
        hi, lo = split(gath[z, q])
        m_hi[q * ch : (q + 1) * ch, :] = hi
        m_lo[q * ch : (q + 1) * ch, :] = lo
    for o in range(1, g):
        a_copy(o).wait_recv()
        hi, lo = split(a_recv[o - 1])
        from_core = lax.rem(c + g - o, g)
        a_hi[from_core] = hi
        a_lo[from_core] = lo

    plain = (((1,), (0,)), ((), ()))

    def process(b, q):
        x = gath[b, q]
        for h in range(g):
            p = product(x, a_hi[h], a_lo[h], plain)
            part[b, q, :, h * cols : (h + 1) * cols] = p

        @pl.when(q == r)
        def _():
            rs[b, r] = part[b, q]

        @pl.when(q != r)
        def _():
            part_copy(b, q).start()

    def add_up(b):
        for o in range(1, n):
            src = lax.rem(r + o, n)
            copy(
                part.at[b, 0], rs.at[b, src], part_sem.at[b, 0], rs_sem.at[b, src], dev(src, z)
            ).wait_recv()
        total = rs[b, 0]
        for s in range(1, n):
            total = total + rs[b, s]
        sums[b] = total
        home = (z == r) & (b == z)

        @pl.when(home)
        def _():
            fin[r] = sums[b]

        @pl.when(jnp.logical_not(home))
        def _():
            sum_copy(b).start()

    @pl.loop(0, n)
    def _(q):
        process(z, q)

    def add_step(d):
        @pl.when(z - d >= 0)
        def _():
            add_up(z - d)

        @pl.when((z + d < nz) & (d > 0))
        def _():
            add_up(z + d)

    @pl.loop(1, nz)
    def _(d):
        @pl.loop(0, n)
        def _(q):
            @pl.when(z - d >= 0)
            def _():
                to_right(z - d, q).wait_recv()

                @pl.when(z < nz - 1)
                def _():
                    to_right(z - d, q).start()

                process(z - d, q)

            @pl.when(z + d < nz)
            def _():
                to_left(z + d, q).wait_recv()

                @pl.when(z > 0)
                def _():
                    to_left(z + d, q).start()

                process(z + d, q)

        add_step(d - 1)

    add_step(nz - 1)

    trans = (((1,), (1,)), ((), ()))

    def dpart_copy(q):
        return copy(dpart.at[q], drecv.at[r], dp_sem.at[q], dr_sem.at[r], dev(q, z))

    @pl.loop(0, n)
    def _(q):
        @pl.when(jnp.logical_not((z == r) & (q == r)))
        def _():
            copy(sums.at[0], fin.at[q], sum_sem.at[0], fin_sem.at[q], dev(q, r)).wait_recv()

        x = -fin[q]
        inv_ref[pl.ds(pl.multiple_of(q * ch, ch), ch), :] = x
        dpart[q] = product(x, m_hi[...], m_lo[...], trans)

        @pl.when(q == r)
        def _():
            drecv[r] = dpart[q]

        @pl.when(q != r)
        def _():
            dpart_copy(q).start()

    for o in range(1, n):
        src = lax.rem(r + o, n)
        copy(dpart.at[0], drecv.at[src], dp_sem.at[0], dr_sem.at[src], dev(src, z)).wait_recv()
    total = drecv[0]
    for s in range(1, n):
        total = total + drecv[s]
    dsum[...] = diag_ref[0, pl.ds(pl.multiple_of(r * ch, ch), ch), :] - total

    def out_copy(o):
        return copy(dsum, dout.at[r], db_sem.at[o - 1], do_sem.at[r], dev(lax.rem(r + o, n), z))

    for o in range(1, n):
        out_copy(o).start()
    out_diag_ref[0, pl.ds(pl.multiple_of(r * ch, ch), ch), :] = dsum[...]

    for o in range(1, g):
        a_copy(o).wait_send()

    @pl.loop(0, nz)
    def _(b):
        @pl.loop(0, n)
        def _(q):
            @pl.when((z < nz - 1) & (b <= z))
            def _():
                to_right(b, q).wait_send()

            @pl.when((z > 0) & (b >= z))
            def _():
                to_left(b, q).wait_send()

            @pl.when(q != r)
            def _():
                part_copy(b, q).wait_send()

        @pl.when(jnp.logical_not((z == r) & (b == z)))
        def _():
            sum_copy(b).wait_send()

    @pl.loop(0, n)
    def _(q):
        @pl.when(q != r)
        def _():
            dpart_copy(q).wait_send()

    for o in range(1, n):
        out_copy(o).wait_send()
    for o in range(1, n):
        src = lax.rem(r + o, n)
        copy(dsum, dout.at[src], db_sem.at[0], do_sem.at[src], dev(src, z)).wait_recv()
        out_diag_ref[0, pl.ds(pl.multiple_of(src * ch, ch), ch), :] = dout[src]


def local(n, npc, panel_t, ancestor, structure, diag_inv):
    _, width, span = panel_t.shape
    cols = ancestor.shape[1]
    g = span // cols
    nz = npc // g
    ch = width // n
    dma = pltpu.SemaphoreType.DMA
    vmem = pl.BlockSpec(memory_space=pltpu.VMEM)
    return pl.pallas_call(
        functools.partial(kernel, n, nz, g),
        out_shape=(
            jax.ShapeDtypeStruct((width, span), f32),
            jax.ShapeDtypeStruct(diag_inv.shape, f32),
        ),
        in_specs=[pl.BlockSpec(memory_space=pltpu.SMEM), vmem, vmem, vmem],
        out_specs=(vmem, vmem),
        scratch_shapes=[
            pltpu.VMEM((nz, n, ch, span), f32),
            pltpu.VMEM((nz, n, ch, span), f32),
            pltpu.VMEM((nz, n, ch, span), f32),
            pltpu.VMEM((nz, ch, span), f32),
            pltpu.VMEM((n, ch, span), f32),
            pltpu.VMEM((g - 1, span, cols), f32),
            pltpu.VMEM((g, span, cols), bf16),
            pltpu.VMEM((g, span, cols), bf16),
            pltpu.VMEM((width, span), bf16),
            pltpu.VMEM((width, span), bf16),
            pltpu.VMEM((n, ch, width), f32),
            pltpu.VMEM((n, ch, width), f32),
            pltpu.VMEM((ch, width), f32),
            pltpu.VMEM((n, ch, width), f32),
            dma((g - 1,)), dma((g - 1,)),
            dma((nz, n)), dma((nz, n)), dma((nz, n)), dma((nz, n)), dma((nz, n)),
            dma((nz,)), dma((n,)),
            dma((n,)), dma((n,)), dma((n - 1,)), dma((n,)),
        ],
        compiler_params=pltpu.CompilerParams(
            collective_id=0, has_side_effects=True, vmem_limit_bytes=60 * 1024 * 1024
        ),
    )(structure, panel_t, ancestor, diag_inv)


def solution(mesh):
    return jax.shard_map(
        functools.partial(local, mesh.shape["prow"], mesh.shape["pcol"]),
        mesh=mesh,
        in_specs=(P("pcol", None, "prow"), P("prow", "pcol"), P(), P("pcol", None, None)),
        out_specs=(P("pcol", "prow"), P("pcol", None, None)),
        check_vma=False,
    )
```

```python
import functools

import jax
import jax.numpy as jnp
from jax import lax
from jax.experimental import pallas as pl
from jax.experimental.pallas import tpu as pltpu
from jax.sharding import PartitionSpec as P

MESH = pl.DeviceIdType.MESH
f32 = jnp.float32
bf16 = jnp.bfloat16


def split(x):
    hi = x.astype(bf16)
    return hi, (x - hi.astype(f32)).astype(bf16)


def product(x, w_hi, w_lo, dims):
    hi, lo = split(x)
    rows = x.shape[0]
    both = lax.dot_general(
        jnp.concatenate([hi, lo], axis=0), w_hi, dims, preferred_element_type=f32
    )
    return both[:rows] + (
        both[rows:] + lax.dot_general(hi, w_lo, dims, preferred_element_type=f32)
    )


def kernel(
    n, nz, g,
    st_ref, panel_ref, anc_ref, diag_ref, inv_ref, out_diag_ref,
    gath, part, rs, sums, fin, a_recv, a_hi, a_lo, m_hi, m_lo, dpart, drecv, dsum, dout,
    pz, ext, rel,
    a_send_sem, a_recv_sem, right_sem, left_sem, gath_sem, part_sem, rs_sem,
    sum_sem, fin_sem, dp_sem, dr_sem, db_sem, do_sem,
    scat_sem, fwd_sem, pz_sem, rel_sem, out_sem,
):
    r = lax.axis_index("prow")
    me = lax.axis_index("pcol")
    z, c = me // g, me % g
    width = panel_ref.shape[1]
    ch = width // n
    nb = panel_ref.shape[2] // width
    cols = anc_ref.shape[1]

    def dev(row, plane):
        return (row, plane * g + c)

    def copy(src, dst, s, d, to):
        return pltpu.make_async_remote_copy(
            src_ref=src, dst_ref=dst, send_sem=s, recv_sem=d, device_id=to, device_id_type=MESH
        )

    barrier = pltpu.get_barrier_semaphore()
    for step in range(1, n * nz):
        other = lax.rem(r * nz + z + step, n * nz)
        pl.semaphore_signal(barrier, inc=1, device_id=dev(other // nz, other % nz), device_id_type=MESH)
    for o in range(1, g):
        pl.semaphore_signal(
            barrier, inc=1, device_id=(r, z * g + lax.rem(c + o, g)), device_id_type=MESH
        )

    mask = [st_ref[me, r * nb + j].astype(f32) for j in range(nb)]
    for q in range(n):
        for j in range(nb):
            at = slice(j * width, (j + 1) * width)
            gath[z, q, :, at] = panel_ref[0, q * ch : (q + 1) * ch, at] * mask[j]

    pl.semaphore_wait(barrier, n * nz - 1 + g - 1)

    def a_copy(o):
        return copy(
            anc_ref, a_recv.at[o - 1], a_send_sem.at[o - 1], a_recv_sem.at[o - 1],
            (r, z * g + lax.rem(c + o, g)),
        )

    for o in range(1, g):
        a_copy(o).start()

    def to_right(b, q):
        return copy(gath.at[b, q], gath.at[b, q], right_sem.at[b, q], gath_sem.at[b, q], dev(r, z + 1))

    def to_left(b, q):
        return copy(gath.at[b, q], gath.at[b, q], left_sem.at[b, q], gath_sem.at[b, q], dev(r, z - 1))

    def part_copy(b, q):
        return copy(part.at[b, q], rs.at[b, r], part_sem.at[b, q], rs_sem.at[b, r], dev(q, z))

    def sum_copy(b):
        return copy(sums.at[b], fin.at[r], sum_sem.at[b], fin_sem.at[r], dev(z, b))

    def detour(b):
        return copy(sums.at[b], rel.at[b], sum_sem.at[b], rel_sem.at[b], dev(z, z))

    def detour_out(b):
        return copy(rel.at[b], fin.at[b], out_sem.at[b], fin_sem.at[b], dev(z, b))

    def scatter(q):
        return copy(gath.at[z, q], pz.at[q], scat_sem.at[q], pz_sem.at[q], dev(q, z))

    def spread(to):
        return copy(pz.at[r], pz.at[r], fwd_sem.at[to], pz_sem.at[r], dev(to, z))

    def spread_all(act):
        for to in range(n):
            @pl.when((r != to) & (z != to))
            def _():
                act(spread(to))

    for q in range(n):
        @pl.when((z < nz - 1) & (z != r))
        def _():
            to_right(z, q).start()

        @pl.when((z > 0) & (z != r))
        def _():
            to_left(z, q).start()

        @pl.when((z == r) & (z != q))
        def _():
            scatter(q).start()

    @pl.when(z == r)
    def _():
        pz[r] = gath[z, r]
        spread_all(lambda d: d.start())

    @pl.loop(0, nz)
    def _(b):
        @pl.when(b != z)
        def _():
            rs[b, b] = jnp.zeros(rs.shape[2:], f32)

    hi, lo = split(anc_ref[...])
    a_hi[c] = hi
    a_lo[c] = lo
    for q in range(n):
        hi, lo = split(gath[z, q])
        m_hi[q * ch : (q + 1) * ch, :] = hi
        m_lo[q * ch : (q + 1) * ch, :] = lo
    for o in range(1, g):
        a_copy(o).wait_recv()
        hi, lo = split(a_recv[o - 1])
        from_core = lax.rem(c + g - o, g)
        a_hi[from_core] = hi
        a_lo[from_core] = lo

    plain = (((1,), (0,)), ((), ()))

    def process(b, q):
        x = gath[b, q]
        for h in range(g):
            p = product(x, a_hi[h], a_lo[h], plain)
            part[b, q, :, h * cols : (h + 1) * cols] = p

        @pl.when(q == r)
        def _():
            rs[b, r] = part[b, q]

        @pl.when(q != r)
        def _():
            part_copy(b, q).start()

    def add_up(b):
        for o in range(1, n):
            src = lax.rem(r + o, n)

            @pl.when((src != b) | (b == z))
            def _():
                copy(
                    part.at[b, 0], rs.at[b, src], part_sem.at[b, 0], rs_sem.at[b, src], dev(src, z)
                ).wait_recv()

        total = rs[b, 0]
        for s in range(1, n):
            total = total + rs[b, s]
        sums[b] = total
        home = (z == r) & (b == z)

        @pl.when(home)
        def _():
            fin[r] = sums[b]

        @pl.when((b != z) & (b == r))
        def _():
            detour(b).start()

        @pl.when(jnp.logical_not(home) & ((b == z) | (b != r)))
        def _():
            sum_copy(b).start()

    def pass_on(b):
        detour(b).wait_recv()
        detour_out(b).start()

    @pl.loop(0, n)
    def _(q):
        process(z, q)

    def add_step(d):
        @pl.when(z - d >= 0)
        def _():
            add_up(z - d)

        @pl.when((z + d < nz) & (d > 0))
        def _():
            add_up(z + d)

    def pass_step(d):
        @pl.when((z == r) & (z - d >= 0) & (d > 0))
        def _():
            pass_on(z - d)

        @pl.when((z == r) & (z + d < nz) & (d > 0))
        def _():
            pass_on(z + d)

    @pl.loop(1, nz)
    def _(d):
        @pl.loop(0, n)
        def _(q):
            @pl.when((z - d >= 0) & (z - d != r))
            def _():
                to_right(z - d, q).wait_recv()

                @pl.when(z < nz - 1)
                def _():
                    to_right(z - d, q).start()

                process(z - d, q)

            @pl.when((z + d < nz) & (z + d != r))
            def _():
                to_left(z + d, q).wait_recv()

                @pl.when(z > 0)
                def _():
                    to_left(z + d, q).start()

                process(z + d, q)

            @pl.when((d == 1) & (q == n // 2) & (r != z))
            def _():
                copy(pz.at[r], pz.at[r], fwd_sem.at[r], pz_sem.at[r], dev(z, z)).wait_recv()
                spread_all(lambda d: d.start())

        add_step(d - 1)
        pass_step(d - 2)

    trans = (((1,), (1,)), ((), ()))

    @pl.loop(0, n)
    def _(q):
        @pl.when(z == r)
        def _():
            ext[q] = jnp.zeros(ext.shape[1:], f32)

        @pl.when(z != r)
        def _():
            @pl.when(q != r)
            def _():
                copy(pz.at[q], pz.at[q], fwd_sem.at[q], pz_sem.at[q], dev(q, z)).wait_recv()

            x = pz[q]
            total = product(x[:, :cols], a_hi[0], a_lo[0], trans)
            for h in range(1, g):
                total = total + product(x[:, h * cols : (h + 1) * cols], a_hi[h], a_lo[h], trans)
            ext[q] = total

    add_step(nz - 1)
    pass_step(nz - 2)
    pass_step(nz - 1)

    def dpart_copy(q):
        return copy(dpart.at[q], drecv.at[r], dp_sem.at[q], dr_sem.at[r], dev(q, z))

    @pl.loop(0, n)
    def _(q):
        @pl.when(jnp.logical_not((z == r) & (q == r)))
        def _():
            copy(sums.at[0], fin.at[q], sum_sem.at[0], fin_sem.at[q], dev(q, r)).wait_recv()

        x = -(fin[q] + ext[q])
        inv_ref[pl.ds(pl.multiple_of(q * ch, ch), ch), :] = x
        dpart[q] = product(x, m_hi[...], m_lo[...], trans)

        @pl.when(q == r)
        def _():
            drecv[r] = dpart[q]

        @pl.when(q != r)
        def _():
            dpart_copy(q).start()

    for o in range(1, n):
        src = lax.rem(r + o, n)
        copy(dpart.at[0], drecv.at[src], dp_sem.at[0], dr_sem.at[src], dev(src, z)).wait_recv()
    total = drecv[0]
    for s in range(1, n):
        total = total + drecv[s]
    dsum[...] = diag_ref[0, pl.ds(pl.multiple_of(r * ch, ch), ch), :] - total

    def out_copy(o):
        return copy(dsum, dout.at[r], db_sem.at[o - 1], do_sem.at[r], dev(lax.rem(r + o, n), z))

    for o in range(1, n):
        out_copy(o).start()
    out_diag_ref[0, pl.ds(pl.multiple_of(r * ch, ch), ch), :] = dsum[...]

    for o in range(1, g):
        a_copy(o).wait_send()

    @pl.loop(0, nz)
    def _(b):
        @pl.loop(0, n)
        def _(q):
            @pl.when((z < nz - 1) & (b <= z) & (b != r))
            def _():
                to_right(b, q).wait_send()

            @pl.when((z > 0) & (b >= z) & (b != r))
            def _():
                to_left(b, q).wait_send()

            @pl.when((q != r) & ((b != r) | (b == z)))
            def _():
                part_copy(b, q).wait_send()

        @pl.when(jnp.logical_not((z == r) & (b == z)))
        def _():
            sum_copy(b).wait_send()

        @pl.when((z == r) & (b != z))
        def _():
            detour_out(b).wait_send()

    @pl.loop(0, n)
    def _(q):
        @pl.when(q != r)
        def _():
            dpart_copy(q).wait_send()

        @pl.when((z == r) & (q != z))
        def _():
            scatter(q).wait_send()

    spread_all(lambda d: d.wait_send())
    for o in range(1, n):
        out_copy(o).wait_send()
    for o in range(1, n):
        src = lax.rem(r + o, n)
        copy(dsum, dout.at[src], db_sem.at[0], do_sem.at[src], dev(src, z)).wait_recv()
        out_diag_ref[0, pl.ds(pl.multiple_of(src * ch, ch), ch), :] = dout[src]


def local(n, npc, panel_t, ancestor, structure, diag_inv):
    _, width, span = panel_t.shape
    cols = ancestor.shape[1]
    g = span // cols
    nz = npc // g
    ch = width // n
    dma = pltpu.SemaphoreType.DMA
    vmem = pl.BlockSpec(memory_space=pltpu.VMEM)
    return pl.pallas_call(
        functools.partial(kernel, n, nz, g),
        out_shape=(
            jax.ShapeDtypeStruct((width, span), f32),
            jax.ShapeDtypeStruct(diag_inv.shape, f32),
        ),
        in_specs=[pl.BlockSpec(memory_space=pltpu.SMEM), vmem, vmem, vmem],
        out_specs=(vmem, vmem),
        scratch_shapes=[
            pltpu.VMEM((nz, n, ch, span), f32),
            pltpu.VMEM((nz, n, ch, span), f32),
            pltpu.VMEM((nz, n, ch, span), f32),
            pltpu.VMEM((nz, ch, span), f32),
            pltpu.VMEM((n, ch, span), f32),
            pltpu.VMEM((g - 1, span, cols), f32),
            pltpu.VMEM((g, span, cols), bf16),
            pltpu.VMEM((g, span, cols), bf16),
            pltpu.VMEM((width, span), bf16),
            pltpu.VMEM((width, span), bf16),
            pltpu.VMEM((n, ch, width), f32),
            pltpu.VMEM((n, ch, width), f32),
            pltpu.VMEM((ch, width), f32),
            pltpu.VMEM((n, ch, width), f32),
            pltpu.VMEM((n, ch, span), f32),
            pltpu.VMEM((n, ch, span), f32),
            pltpu.VMEM((nz, ch, span), f32),
            dma((g - 1,)), dma((g - 1,)),
            dma((nz, n)), dma((nz, n)), dma((nz, n)), dma((nz, n)), dma((nz, n)),
            dma((nz,)), dma((n,)),
            dma((n,)), dma((n,)), dma((n - 1,)), dma((n,)),
            dma((n,)), dma((n,)), dma((n,)), dma((nz,)), dma((nz,)),
        ],
        compiler_params=pltpu.CompilerParams(
            collective_id=0, has_side_effects=True, vmem_limit_bytes=60 * 1024 * 1024
        ),
    )(structure, panel_t, ancestor, diag_inv)


def solution(mesh):
    return jax.shard_map(
        functools.partial(local, mesh.shape["prow"], mesh.shape["pcol"]),
        mesh=mesh,
        in_specs=(P("pcol", None, "prow"), P("prow", "pcol"), P(), P("pcol", None, None)),
        out_specs=(P("pcol", "prow"), P("pcol", None, None)),
        check_vma=False,
    )
```

```python
import functools

import jax
import jax.numpy as jnp
from jax import lax
from jax.experimental import pallas as pl
from jax.experimental.pallas import tpu as pltpu
from jax.sharding import PartitionSpec as P

MESH = pl.DeviceIdType.MESH
f32 = jnp.float32
bf16 = jnp.bfloat16


def split(x):
    hi = x.astype(bf16)
    return hi, (x - hi.astype(f32)).astype(bf16)


def product(x, w_hi, w_lo, dims):
    hi, lo = split(x)
    rows = x.shape[0]
    both = lax.dot_general(
        jnp.concatenate([hi, lo], axis=0), w_hi, dims, preferred_element_type=f32
    )
    return both[:rows] + (
        both[rows:] + lax.dot_general(hi, w_lo, dims, preferred_element_type=f32)
    )


def kernel(
    n, nz, g,
    st_ref, panel_ref, anc_ref, diag_ref, inv_ref, out_diag_ref,
    gath, part, rs, sums, fin, a_recv, a_hi, a_lo, m_hi, m_lo, dpart, drecv, dsum, dout,
    pz, ext,
    a_send_sem, a_recv_sem, right_sem, left_sem, gath_sem, part_sem, rs_sem,
    sum_sem, fin_sem, dp_sem, dr_sem, db_sem, do_sem,
    scat_sem, fwd_sem, pz_sem,
):
    r = lax.axis_index("prow")
    me = lax.axis_index("pcol")
    z, c = me // g, me % g
    width = panel_ref.shape[1]
    ch = width // n
    nb = panel_ref.shape[2] // width
    cols = anc_ref.shape[1]

    def dev(row, plane):
        return (row, plane * g + c)

    def copy(src, dst, s, d, to):
        return pltpu.make_async_remote_copy(
            src_ref=src, dst_ref=dst, send_sem=s, recv_sem=d, device_id=to, device_id_type=MESH
        )

    barrier = pltpu.get_barrier_semaphore()
    for step in range(1, n * nz):
        other = lax.rem(r * nz + z + step, n * nz)
        pl.semaphore_signal(barrier, inc=1, device_id=dev(other // nz, other % nz), device_id_type=MESH)
    for o in range(1, g):
        pl.semaphore_signal(
            barrier, inc=1, device_id=(r, z * g + lax.rem(c + o, g)), device_id_type=MESH
        )

    mask = [st_ref[me, r * nb + j].astype(f32) for j in range(nb)]
    for q in range(n):
        for j in range(nb):
            at = slice(j * width, (j + 1) * width)
            gath[z, q, :, at] = panel_ref[0, q * ch : (q + 1) * ch, at] * mask[j]

    pl.semaphore_wait(barrier, n * nz - 1 + g - 1)

    def a_copy(o):
        return copy(
            anc_ref, a_recv.at[o - 1], a_send_sem.at[o - 1], a_recv_sem.at[o - 1],
            (r, z * g + lax.rem(c + o, g)),
        )

    for o in range(1, g):
        a_copy(o).start()

    def to_right(b, q):
        return copy(gath.at[b, q], gath.at[b, q], right_sem.at[b, q], gath_sem.at[b, q], dev(r, z + 1))

    def to_left(b, q):
        return copy(gath.at[b, q], gath.at[b, q], left_sem.at[b, q], gath_sem.at[b, q], dev(r, z - 1))

    def part_copy(b, q):
        return copy(part.at[b, q], rs.at[b, r], part_sem.at[b, q], rs_sem.at[b, r], dev(q, z))

    def sum_copy(b):
        return copy(sums.at[b], fin.at[r], sum_sem.at[b], fin_sem.at[r], dev(z, b))

    def scatter(q):
        return copy(gath.at[z, q], pz.at[q], scat_sem.at[q], pz_sem.at[q], dev(q, z))

    def spread(to):
        return copy(pz.at[r], pz.at[r], fwd_sem.at[to], pz_sem.at[r], dev(to, z))

    def spread_all(act):
        for to in range(n):
            @pl.when((r != to) & (z != to))
            def _():
                act(spread(to))

    for q in range(n):
        @pl.when((z < nz - 1) & (z != r))
        def _():
            to_right(z, q).start()

        @pl.when((z > 0) & (z != r))
        def _():
            to_left(z, q).start()

    @pl.loop(0, nz)
    def _(b):
        @pl.when(b != z)
        def _():
            rs[b, b] = jnp.zeros(rs.shape[2:], f32)

    hi, lo = split(anc_ref[...])
    a_hi[c] = hi
    a_lo[c] = lo
    for q in range(n):
        hi, lo = split(gath[z, q])
        m_hi[q * ch : (q + 1) * ch, :] = hi
        m_lo[q * ch : (q + 1) * ch, :] = lo
    for o in range(1, g):
        a_copy(o).wait_recv()
        hi, lo = split(a_recv[o - 1])
        from_core = lax.rem(c + g - o, g)
        a_hi[from_core] = hi
        a_lo[from_core] = lo

    plain = (((1,), (0,)), ((), ()))

    def process(b, q):
        x = gath[b, q]
        for h in range(g):
            p = product(x, a_hi[h], a_lo[h], plain)
            part[b, q, :, h * cols : (h + 1) * cols] = p

        @pl.when(q == r)
        def _():
            rs[b, r] = part[b, q]

        @pl.when(q != r)
        def _():
            part_copy(b, q).start()

    def add_up(b):
        for o in range(1, n):
            src = lax.rem(r + o, n)

            @pl.when((src != b) | (b == z))
            def _():
                copy(
                    part.at[b, 0], rs.at[b, src], part_sem.at[b, 0], rs_sem.at[b, src], dev(src, z)
                ).wait_recv()

        total = rs[b, 0]
        for s in range(1, n):
            total = total + rs[b, s]
        sums[b] = total
        home = (z == r) & (b == z)

        @pl.when(home)
        def _():
            fin[r] = sums[b]

        @pl.when(jnp.logical_not(home))
        def _():
            sum_copy(b).start()

    @pl.loop(0, n)
    def _(q):
        process(z, q)

    @pl.when(z == r)
    def _():
        for q in range(n):
            @pl.when(z != q)
            def _():
                scatter(q).start()

        pz[r] = gath[z, r]
        spread_all(lambda d: d.start())

    def add_step(d):
        @pl.when(z - d >= 0)
        def _():
            add_up(z - d)

        @pl.when((z + d < nz) & (d > 0))
        def _():
            add_up(z + d)

    @pl.loop(1, nz)
    def _(d):
        @pl.loop(0, n)
        def _(q):
            @pl.when((z - d >= 0) & (z - d != r))
            def _():
                to_right(z - d, q).wait_recv()

                @pl.when(z < nz - 1)
                def _():
                    to_right(z - d, q).start()

                process(z - d, q)

            @pl.when((z + d < nz) & (z + d != r))
            def _():
                to_left(z + d, q).wait_recv()

                @pl.when(z > 0)
                def _():
                    to_left(z + d, q).start()

                process(z + d, q)

            @pl.when((d == min(2, nz - 1)) & (q == 0) & (r != z))
            def _():
                copy(pz.at[r], pz.at[r], fwd_sem.at[r], pz_sem.at[r], dev(z, z)).wait_recv()
                spread_all(lambda d: d.start())

        add_step(d - 1)

    trans = (((1,), (1,)), ((), ()))

    @pl.loop(0, n)
    def _(q):
        @pl.when(z == r)
        def _():
            ext[q] = jnp.zeros(ext.shape[1:], f32)

        @pl.when(z != r)
        def _():
            @pl.when(q != r)
            def _():
                copy(pz.at[q], pz.at[q], fwd_sem.at[q], pz_sem.at[q], dev(q, z)).wait_recv()

            x = pz[q]
            total = product(x[:, :cols], a_hi[0], a_lo[0], trans)
            for h in range(1, g):
                total = total + product(x[:, h * cols : (h + 1) * cols], a_hi[h], a_lo[h], trans)
            ext[q] = total

    add_step(nz - 1)

    def dpart_copy(q):
        return copy(dpart.at[q], drecv.at[r], dp_sem.at[q], dr_sem.at[r], dev(q, z))

    @pl.loop(0, n)
    def _(q):
        @pl.when(jnp.logical_not((z == r) & (q == r)))
        def _():
            copy(sums.at[0], fin.at[q], sum_sem.at[0], fin_sem.at[q], dev(q, r)).wait_recv()

        x = -(fin[q] + ext[q])
        inv_ref[pl.ds(pl.multiple_of(q * ch, ch), ch), :] = x
        dpart[q] = product(x, m_hi[...], m_lo[...], trans)

        @pl.when(q == r)
        def _():
            drecv[r] = dpart[q]

        @pl.when(q != r)
        def _():
            dpart_copy(q).start()

    for o in range(1, n):
        src = lax.rem(r + o, n)
        copy(dpart.at[0], drecv.at[src], dp_sem.at[0], dr_sem.at[src], dev(src, z)).wait_recv()
    total = drecv[0]
    for s in range(1, n):
        total = total + drecv[s]
    dsum[...] = diag_ref[0, pl.ds(pl.multiple_of(r * ch, ch), ch), :] - total

    def out_copy(o):
        return copy(dsum, dout.at[r], db_sem.at[o - 1], do_sem.at[r], dev(lax.rem(r + o, n), z))

    for o in range(1, n):
        out_copy(o).start()
    out_diag_ref[0, pl.ds(pl.multiple_of(r * ch, ch), ch), :] = dsum[...]

    for o in range(1, g):
        a_copy(o).wait_send()

    @pl.loop(0, nz)
    def _(b):
        @pl.loop(0, n)
        def _(q):
            @pl.when((z < nz - 1) & (b <= z) & (b != r))
            def _():
                to_right(b, q).wait_send()

            @pl.when((z > 0) & (b >= z) & (b != r))
            def _():
                to_left(b, q).wait_send()

            @pl.when((q != r) & ((b != r) | (b == z)))
            def _():
                part_copy(b, q).wait_send()

        @pl.when(jnp.logical_not((z == r) & (b == z)))
        def _():
            sum_copy(b).wait_send()

    @pl.loop(0, n)
    def _(q):
        @pl.when(q != r)
        def _():
            dpart_copy(q).wait_send()

        @pl.when((z == r) & (q != z))
        def _():
            scatter(q).wait_send()

    spread_all(lambda d: d.wait_send())
    for o in range(1, n):
        out_copy(o).wait_send()
    for o in range(1, n):
        src = lax.rem(r + o, n)
        copy(dsum, dout.at[src], db_sem.at[0], do_sem.at[src], dev(src, z)).wait_recv()
        out_diag_ref[0, pl.ds(pl.multiple_of(src * ch, ch), ch), :] = dout[src]


def local(n, npc, panel_t, ancestor, structure, diag_inv):
    _, width, span = panel_t.shape
    cols = ancestor.shape[1]
    g = span // cols
    nz = npc // g
    ch = width // n
    dma = pltpu.SemaphoreType.DMA
    vmem = pl.BlockSpec(memory_space=pltpu.VMEM)
    return pl.pallas_call(
        functools.partial(kernel, n, nz, g),
        out_shape=(
            jax.ShapeDtypeStruct((width, span), f32),
            jax.ShapeDtypeStruct(diag_inv.shape, f32),
        ),
        in_specs=[pl.BlockSpec(memory_space=pltpu.SMEM), vmem, vmem, vmem],
        out_specs=(vmem, vmem),
        scratch_shapes=[
            pltpu.VMEM((nz, n, ch, span), f32),
            pltpu.VMEM((nz, n, ch, span), f32),
            pltpu.VMEM((nz, n, ch, span), f32),
            pltpu.VMEM((nz, ch, span), f32),
            pltpu.VMEM((n, ch, span), f32),
            pltpu.VMEM((g - 1, span, cols), f32),
            pltpu.VMEM((g, span, cols), bf16),
            pltpu.VMEM((g, span, cols), bf16),
            pltpu.VMEM((width, span), bf16),
            pltpu.VMEM((width, span), bf16),
            pltpu.VMEM((n, ch, width), f32),
            pltpu.VMEM((n, ch, width), f32),
            pltpu.VMEM((ch, width), f32),
            pltpu.VMEM((n, ch, width), f32),
            pltpu.VMEM((n, ch, span), f32),
            pltpu.VMEM((n, ch, span), f32),
            dma((g - 1,)), dma((g - 1,)),
            dma((nz, n)), dma((nz, n)), dma((nz, n)), dma((nz, n)), dma((nz, n)),
            dma((nz,)), dma((n,)),
            dma((n,)), dma((n,)), dma((n - 1,)), dma((n,)),
            dma((n,)), dma((n,)), dma((n,)),
        ],
        compiler_params=pltpu.CompilerParams(
            collective_id=0, has_side_effects=True, vmem_limit_bytes=60 * 1024 * 1024
        ),
    )(structure, panel_t, ancestor, diag_inv)


def solution(mesh):
    return jax.shard_map(
        functools.partial(local, mesh.shape["prow"], mesh.shape["pcol"]),
        mesh=mesh,
        in_specs=(P("pcol", None, "prow"), P("prow", "pcol"), P(), P("pcol", None, None)),
        out_specs=(P("pcol", "prow"), P("pcol", None, None)),
        check_vma=False,
    )
```
